32 devices in a mesh: replica: 8 (over z, y), fsdp: 4 (over x, core).
Axes of the slice: x: 2, y: 2, z: 4, core: 2. Of those that a mesh axis runs over, the one named last changes fastest.
Arguments:
- activations: bfloat16 [8, 4096, 4096], P('replica', 'fsdp')
- cotangents: bfloat16 [8, 4096, 512], P('replica', 'fsdp'), may hold values from -0.059814453 to 0.059814453
- momentum: float32 [8, 4096, 512], P('replica', 'fsdp'), may hold values from -6 to 6
- keep_index: int32 [8, 512, 32], P(None, 'fsdp'), may hold values from 0 to 4095, as said below
Outputs:
- new_momentum: float32 [8, 4096, 512], P('replica', 'fsdp')
- update: bfloat16 [4096, 512], P('fsdp')
The draws below stay inside these ranges and needn't reach their ends.
Inputs may be any that keep to these rules, and one draw needn't show every extreme that they name: keep_index[r, t, j] lies in [j * 64 * 2, (j + 1) * 64 * 2), so a tile's indices are distinct and ascending.
All inputs are finite; a program needn't handle non-finite values.
Results may differ from the reference program's by a relative error of at most 0.013.
Values may be sent and summed in bfloat16 or wider, within the bound.
No kernel may reach another device: no remote copies, remote signals or barrier semaphores. Data moves between devices by JAX's collectives and lax.ppermute only.
A program may use at most 128 MiB of HBM per device.

```python
import math
import jax
import jax.numpy as jnp
from jax import lax

D_WIN = 4096
KV_WIN = 512
TILE = 64
KEEP = 32
REPLICAS = 8
TOK_REP = 4096
TILES = 512


def draw_activations(key, part):
    key_scale = jax.random.fold_in(key, 11)
    key_value = jax.random.fold_in(key, 12)
    column_scale = jnp.exp(jax.random.uniform(key_scale, (D_WIN,), jnp.float32, 0.0, math.log(10.0)))
    values = jax.random.normal(key_value, (REPLICAS, TOK_REP, D_WIN), jnp.float32)
    return (values * column_scale).astype(jnp.bfloat16)


def draw_keep_index(key, part):
    band = TILE * TILE // KEEP
    offsets = jax.random.randint(jax.random.fold_in(key, 21), (REPLICAS, TILES, KEEP), 0, band, jnp.int32)
    return offsets + jnp.arange(KEEP).astype(jnp.int32) * band


def levels(stream_key, dims, split, smallest, top_value):
    loudness = 1.0
    for dim, parts in split:
        draws = jax.random.uniform(jax.random.fold_in(jax.random.fold_in(stream_key, 6), dim), (parts,), jnp.float32, smallest / len(split), top_value / len(split))
        loudness = loudness * jnp.repeat(jnp.exp(draws), dims[dim] // parts).reshape((-1,) + (1,) * (len(dims) - 1 - dim))
    return loudness


def normal_values(key, extent, deviation, limit, split=(), dtype=jnp.bfloat16):
    gain = levels(key, extent, split, -0.22, 0.18) if split else 1.0
    result = jax.random.normal(key, extent, jnp.float32) * deviation * gain
    return jnp.minimum(jnp.maximum(result, -limit), limit).astype(dtype)


def setup_inputs(seed: int = 0) -> dict:
    key_list = jax.random.split(jax.random.key(seed), 5)
    activations = draw_activations(jax.random.fold_in(key_list[4], 71), 0)
    cotangents = normal_values(key_list[1], (REPLICAS, TOK_REP, KV_WIN), 0.01, 0.059814453, ((0, 8), (1, 4)))
    momentum = normal_values(key_list[2], (REPLICAS, D_WIN, KV_WIN), 1.0, 6.0, ((0, 8), (1, 4)), jnp.float32)
    keep_index = draw_keep_index(jax.random.fold_in(key_list[4], 71), 0)
    return {"activations": activations, "cotangents": cotangents, "momentum": momentum, "keep_index": keep_index}


BETA = 0.999
EPS = 1e-06
highest = lax.Precision.HIGHEST

def cosine_table():
    sample = jnp.arange(TILE).astype(jnp.float32)
    freq_index = sample[:, None]
    table = jnp.cos(jnp.pi * (2.0 * sample[None, :] + 1.0) * freq_index / (2.0 * TILE))
    weight_row = jnp.where(freq_index == 0, jnp.sqrt(1.0 / TILE), jnp.sqrt(2.0 / TILE))
    return (table * weight_row).astype(jnp.float32)

def forward_tiles(matrix, cosine):
    row_count, col_count = matrix.shape
    blocks = matrix.reshape(row_count // TILE, TILE, col_count // TILE, TILE)
    left = jnp.einsum('ka,iajb->ikjb', cosine, blocks, precision=highest)
    return jnp.einsum('ikjb,lb->ikjl', left, cosine, precision=highest).reshape(row_count, col_count)

def inverse_tiles(matrix, cosine):
    row_count, col_count = matrix.shape
    blocks = matrix.reshape(row_count // TILE, TILE, col_count // TILE, TILE)
    left = jnp.einsum('ka,ikjl->iajl', cosine, blocks, precision=highest)
    return jnp.einsum('iajl,lb->iajb', left, cosine, precision=highest).reshape(row_count, col_count)

def flat_positions(indices, col_count):
    tile_count = indices.shape[-2]
    tile_cols = col_count // TILE
    tile_id = jnp.arange(tile_count).astype(jnp.int32)[:, None]
    tile_row = tile_id // tile_cols
    tile_col = tile_id % tile_cols
    freq_row = indices // TILE
    freq_col = indices % TILE
    return ((tile_row * TILE + freq_row) * tile_cols + tile_col) * TILE + freq_col

def reference(activations, cotangents, momentum, keep_index):
    cosine = cosine_table()

    def one_replica(running, inputs):
        tokens_here, grads_here, moment_old, indices = inputs
        gradient = lax.dot_general(tokens_here, grads_here, (((0,), (0,)), ((), ())), preferred_element_type=jnp.float32)
        moment = BETA * moment_old + gradient
        spectrum = forward_tiles(moment, cosine).reshape(-1)
        where_flat = flat_positions(indices, KV_WIN).reshape(-1)
        sent_grid = jnp.zeros_like(spectrum).at[where_flat].add(spectrum[where_flat])
        new_moment = moment - inverse_tiles(sent_grid.reshape(moment.shape), cosine)
        return (running + sent_grid, new_moment)
    start_sum = jnp.zeros((D_WIN * KV_WIN,), jnp.float32)
    summed, new_momentum = lax.scan(one_replica, start_sum, (activations, cotangents, momentum, keep_index))
    merged = inverse_tiles(summed.reshape(D_WIN, KV_WIN), cosine) / REPLICAS
    square_total = jnp.sum(merged * merged)
    scale_factor = lax.rsqrt(square_total / (D_WIN * KV_WIN) + EPS)
    return (new_momentum, (merged * scale_factor).astype(jnp.bfloat16))
```

```python
import functools

import jax
import jax.numpy as jnp
import numpy as np
from jax import lax
from jax.experimental import pallas as pl
from jax.experimental.pallas import tpu as pltpu
from jax.sharding import PartitionSpec as P

TILE = 64
KEEP = 32
BAND = TILE * TILE // KEEP
GROUP = 256
PER = GROUP // TILE
BETA = 0.999
EPS = 1e-06

bf16 = jnp.bfloat16
f32 = jnp.float32
MIB = 1 << 20
VMEM = pl.BlockSpec(memory_space=pltpu.VMEM)
SMEM = pl.BlockSpec(memory_space=pltpu.SMEM)
HBM = pl.BlockSpec(memory_space=pltpu.HBM)
LANES = 128
SUBLANES = 8

FIRST_MIB = 56


def cosine_table():
    n = np.arange(TILE, dtype=np.float64)
    table = np.cos(np.pi * (2.0 * n[None, :] + 1.0) * n[:, None] / (2.0 * TILE))
    return table * np.where(n[:, None] == 0, np.sqrt(1.0 / TILE), np.sqrt(2.0 / TILE))


def halves(matrix):
    high = matrix.astype(np.float32).astype(bf16)
    low = (matrix - np.asarray(high, np.float64)).astype(np.float32).astype(bf16)
    return np.stack([high, low])


def tables():
    cosine = cosine_table()
    order = np.concatenate([np.arange(0, TILE, 2), np.arange(1, TILE, 2)])
    rows = np.kron(np.eye(PER), cosine)
    cols = np.kron(np.eye(PER), cosine[order].T)
    return halves(rows), halves(cols), halves(rows.T.copy())


def split(x):
    high = x.astype(bf16)
    return high, (x - high.astype(f32)).astype(bf16)


def mdot(a, b):
    return jnp.dot(a, b, preferred_element_type=f32)


def ndot(a, b):
    return lax.dot_general(a, b, (((1,), (1,)), ((), ())), preferred_element_type=f32)


def product(dot, a, b):
    out = dot(a[0], b[0]) + dot(a[1], b[0])
    return out if len(b) == 1 else out + dot(a[0], b[1])


def forward_group(x, rows, cols):
    high, low = split(product(ndot, rows, x))
    return mdot(high, cols[0]) + mdot(low, cols[0]) + mdot(high, cols[1])


def inverse_group(spectrum, rows_t, cols):
    return product(ndot, cols, split(product(mdot, rows_t, split(spectrum))))


def lane_block(shape):
    return lax.broadcasted_iota(jnp.int32, shape, len(shape) - 1) // KEEP


def offset_rows(index):
    value = (index & (BAND - 1)).astype(f32)
    value = jnp.concatenate([value] * (LANES // KEEP), axis=0).T
    value = value.reshape(-1, 2, SUBLANES, LANES)
    block = lane_block((value.shape[0], SUBLANES, LANES))
    return jnp.where(block < 2, value[:, 0], value[:, 1]) - jnp.where(block % 2 == 1, float(TILE), 0.0)


def packed(rows):
    rows = rows.reshape(-1, 2, SUBLANES, LANES)
    even, odd = rows[:, 0], rows[:, 1]
    axis = even.ndim - 1
    even = even + pltpu.roll(even, KEEP, axis)
    odd = odd + pltpu.roll(odd, KEEP, axis)
    return jnp.where(lane_block(even.shape) % 2 == 1, even, pltpu.roll(odd, LANES - KEEP, axis))


def unpacked(rows):
    axis = rows.ndim - 1
    upper = lane_block(rows.shape) % 2 == 1
    even = jnp.where(upper, rows, pltpu.roll(rows, LANES - KEEP, axis))
    odd = jnp.where(upper, pltpu.roll(rows, KEEP, axis), rows)
    return even, odd


def row_iota():
    return lax.broadcasted_iota(jnp.int32, (TILE, LANES), 0).astype(f32)


def params(mib):
    return pltpu.CompilerParams(vmem_limit_bytes=mib * MIB)


def cost(flops, bytes_accessed):
    return pl.CostEstimate(flops=flops, bytes_accessed=bytes_accessed, transcendentals=0)


def outer(a, c):
    return lax.dot_general(a, c, (((0,), (0,)), ((), ())), preferred_element_type=f32)


def first_kernel(mine, a_ref, c_ref, o_ref, far, tokens, far_sem, c_sem):
    half = o_ref.shape[0] // 2
    start = (mine[0] ^ 3) * o_ref.shape[0]
    cotangents = pltpu.make_async_copy(c_ref, tokens, c_sem)
    parts = [
        pltpu.make_async_copy(
            a_ref.at[:, pl.ds(pl.multiple_of(start + i * half, LANES), half)], far.at[i], far_sem.at[i]
        )
        for i in range(2)
    ]
    for copy in [cotangents] + parts:
        copy.start()
    cotangents.wait()
    for i, copy in enumerate(parts):
        copy.wait()
        o_ref[i * half : (i + 1) * half, :] = outer(far[i], tokens[...]).astype(bf16)


def first_product(mine, activations, cotangents, rows):
    tokens, kv = cotangents.shape
    return pl.pallas_call(
        first_kernel,
        in_specs=[SMEM, HBM, HBM],
        out_specs=VMEM,
        out_shape=jax.ShapeDtypeStruct((rows, kv), bf16),
        scratch_shapes=[
            pltpu.VMEM((2, tokens, rows // 2), bf16),
            pltpu.VMEM((tokens, kv), bf16),
            pltpu.SemaphoreType.DMA((2,)),
            pltpu.SemaphoreType.DMA,
        ],
        compiler_params=params(FIRST_MIB),
        cost_estimate=cost(2 * tokens * rows * kv, tokens * rows * 2),
        name="first_product",
    )(mine, activations, cotangents)


def product_kernel(distance, mine, a_ref, c_ref, o_ref):
    half = o_ref.shape[0] // 2
    start = (mine[0] ^ distance) * o_ref.shape[0]
    for i in range(2):
        columns = pl.ds(pl.multiple_of(start + i * half, LANES), half)
        o_ref[i * half : (i + 1) * half, :] = outer(a_ref[:, columns], c_ref[...]).astype(o_ref.dtype)


def held_product(distance, mine, activations, cotangents, rows, dtype):
    tokens, kv = cotangents.shape
    return pl.pallas_call(
        functools.partial(product_kernel, distance),
        in_specs=[SMEM, VMEM, VMEM],
        out_specs=VMEM,
        out_shape=jax.ShapeDtypeStruct((rows, kv), dtype),
        compiler_params=params(12),
        cost_estimate=cost(2 * tokens * rows * kv, tokens * rows * 2),
        name="held_product",
    )(mine, activations, cotangents)


def add_kernel(x_ref, y_ref, *o_refs):
    row = 0
    for o_ref in o_refs:
        end = row + o_ref.shape[0]
        o_ref[...] = (x_ref[row:end, :] + y_ref[row:end, :].astype(f32)).astype(bf16)
        row = end


def add_round(x, y, pieces):
    rows, kv = x.shape
    return pl.pallas_call(
        add_kernel,
        in_specs=[VMEM, VMEM],
        out_specs=[VMEM] * len(pieces),
        out_shape=[jax.ShapeDtypeStruct((n, kv), bf16) for n in pieces],
        compiler_params=params(4),
        cost_estimate=cost(rows * kv * 400, rows * kv * 8),
        name="chip_sum",
    )(x, y)


def pick(spectrum, row, col, offset_ref, rows_ref):
    line = row_iota()
    for pair in range(GROUP // LANES):
        for tile in range(PER):
            at = (row // LANES + pair) * SUBLANES + col // TILE + tile
            part = spectrum[tile * TILE : (tile + 1) * TILE, pair * LANES : (pair + 1) * LANES]
            part = jnp.where(offset_ref[at : at + 1, :] == line, part, 0.0)
            rows_ref[at : at + 1, :] = jnp.sum(part, axis=0, keepdims=True)


def kept_cross_kernel(index_ref, row_ref, col_ref, *refs):
    *x_refs, o_ref, offset_ref, rows_ref = refs
    offset_ref[...] = offset_rows(index_ref[...]).reshape(offset_ref.shape)
    first = 0
    for x_ref in x_refs:
        for row in range(0, x_ref.shape[0], GROUP):
            for col in range(0, x_ref.shape[1], GROUP):
                x = x_ref[row : row + GROUP, col : col + GROUP]
                pick(forward_group((x,), row_ref, col_ref), first + row, col, offset_ref, rows_ref)
        first += x_ref.shape[0]
    o_ref[...] = packed(rows_ref[...]).reshape(o_ref.shape)


def row_scratch(tiles, count=None):
    shape = (tiles // 2, LANES)
    return pltpu.VMEM(shape if count is None else (count, *shape), f32)


def kept_cross(pieces, index, rows, cols):
    tiles = index.shape[1]
    return pl.pallas_call(
        kept_cross_kernel,
        in_specs=[VMEM] * (3 + len(pieces)),
        out_specs=VMEM,
        out_shape=jax.ShapeDtypeStruct((tiles // 4, LANES), f32),
        scratch_shapes=[row_scratch(tiles), row_scratch(tiles)],
        compiler_params=params(8),
        cost_estimate=cost(2 * 10**9, MIB),
        name="kept_cross",
    )(index, rows, cols, *pieces)


def kept_own_kernel(x_ref, y_ref, momentum_ref, index_ref, cross_ref, row_ref, col_ref, moment_ref, o_ref, offset_ref, rows_ref):
    offset_ref[...] = offset_rows(index_ref[...]).reshape(offset_ref.shape)
    for row in range(0, x_ref.shape[0], GROUP):
        for col in range(0, x_ref.shape[1], GROUP):
            at = (slice(row, row + GROUP), slice(col, col + GROUP))
            x = x_ref[at] + y_ref[at].astype(f32) + BETA * momentum_ref[at]
            moment_ref[at] = x
            pick(forward_group(split(x), row_ref, col_ref), row, col, offset_ref, rows_ref)
    o_ref[...] = cross_ref[...] + packed(rows_ref[...]).reshape(o_ref.shape)


def kept_own(partial, received, momentum, index, cross, rows, cols):
    tiles = index.shape[1]
    return pl.pallas_call(
        kept_own_kernel,
        in_specs=[VMEM] * 7,
        out_specs=[VMEM, VMEM],
        out_shape=[jax.ShapeDtypeStruct(partial.shape, f32), jax.ShapeDtypeStruct(cross.shape, f32)],
        scratch_shapes=[row_scratch(tiles), row_scratch(tiles)],
        compiler_params=params(8),
        cost_estimate=cost(2 * 10**9, 4 * MIB),
        name="kept_own",
    )(partial, received, momentum, index, cross, rows, cols)


def store_unpacked(packed_rows, to_ref):
    rows = packed_rows.reshape(-1, SUBLANES, LANES)
    even, odd = unpacked(rows)
    for i in range(rows.shape[0]):
        to_ref[2 * i * SUBLANES : (2 * i + 1) * SUBLANES, :] = even[i]
        to_ref[(2 * i + 1) * SUBLANES : (2 * i + 2) * SUBLANES, :] = odd[i]


def drop_sent_kernel(moment_ref, kept_ref, index_ref, row_t_ref, col_ref, o_ref, offset_ref, value_ref):
    offset_ref[...] = offset_rows(index_ref[...]).reshape(offset_ref.shape)
    store_unpacked(kept_ref[...], value_ref)
    line = row_iota()
    for row in range(0, moment_ref.shape[0], GROUP):
        for col in range(0, moment_ref.shape[1], GROUP):
            lanes = []
            for pair in range(GROUP // LANES):
                first = (row // LANES + pair) * SUBLANES + col // TILE
                lanes.append(
                    jnp.concatenate(
                        [
                            jnp.where(offset_ref[i : i + 1, :] == line, value_ref[i : i + 1, :], 0.0)
                            for i in range(first, first + PER)
                        ],
                        axis=0,
                    )
                )
            at = (slice(row, row + GROUP), slice(col, col + GROUP))
            o_ref[at] = moment_ref[at] - inverse_group(jnp.concatenate(lanes, axis=1), row_t_ref, col_ref)


def drop_sent(moment, kept, index, rows_t, cols):
    tiles = index.shape[1]
    return pl.pallas_call(
        drop_sent_kernel,
        in_specs=[VMEM] * 5,
        out_specs=VMEM,
        out_shape=jax.ShapeDtypeStruct(moment.shape, f32),
        scratch_shapes=[row_scratch(tiles), row_scratch(tiles)],
        compiler_params=params(8),
        cost_estimate=cost(2 * 10**9, 4 * MIB),
        name="drop_sent",
    )(moment, kept, index, rows_t, cols)


def sum_kernel(counts, me_ref, index_ref, *refs):
    *kept_refs, o_ref, square_ref, offset_ref, value_ref = refs
    replicas = sum(counts)
    slot = 0
    for kept_ref, count in zip(kept_refs, counts):
        for i in range(count):
            index = index_ref[me_ref[0] ^ slot]
            offset_ref[slot] = offset_rows(index).reshape(offset_ref.shape[1:])
            store_unpacked(kept_ref[i], value_ref.at[slot])
            slot += 1
    line = row_iota()
    squares = jnp.zeros((TILE, LANES), f32)
    for pair in range(o_ref.shape[1] // LANES):
        for tile in range(o_ref.shape[0] // TILE):
            at = pair * SUBLANES + tile

            def add(slot, total):
                return total + jnp.where(
                    offset_ref[slot, at : at + 1, :] == line, value_ref[slot, at : at + 1, :], 0.0
                )

            total = lax.fori_loop(0, replicas, add, jnp.zeros((TILE, LANES), f32), unroll=min(replicas, 8))
            o_ref[tile * TILE : (tile + 1) * TILE, pair * LANES : (pair + 1) * LANES] = total
            squares += total * total
    total = jnp.sum(squares, axis=0, keepdims=True)
    square_ref[...] = jnp.broadcast_to(jnp.sum(total, axis=1, keepdims=True), square_ref.shape)


def sum_replicas(me, index, pieces, rows, kv):
    tiles = index.shape[2]
    counts = [piece.shape[0] for piece in pieces]
    return pl.pallas_call(
        functools.partial(sum_kernel, counts),
        in_specs=[SMEM] + [VMEM] * (1 + len(pieces)),
        out_specs=[VMEM, VMEM],
        out_shape=[jax.ShapeDtypeStruct((kv, rows), f32), jax.ShapeDtypeStruct((SUBLANES, LANES), f32)],
        scratch_shapes=[row_scratch(tiles, sum(counts)), row_scratch(tiles, sum(counts))],
        compiler_params=params(12),
        cost_estimate=cost(3 * 10**9, 4 * MIB),
        name="sum_replicas",
    )(me, index, *pieces)


def inverse_kernel(x_ref, row_t_ref, col_ref, o_ref):
    for row in range(0, o_ref.shape[0], GROUP):
        for col in range(0, o_ref.shape[1], GROUP):
            at = (slice(row, row + GROUP), slice(col, col + GROUP))
            o_ref[at] = inverse_group(x_ref[at[1], at[0]], row_t_ref, col_ref)


def inverse(x, rows_t, cols):
    return pl.pallas_call(
        inverse_kernel,
        in_specs=[VMEM] * 3,
        out_specs=VMEM,
        out_shape=jax.ShapeDtypeStruct(x.shape[::-1], f32),
        compiler_params=params(8),
        cost_estimate=cost(2 * 10**9, 4 * MIB),
        name="inverse",
    )(x, rows_t, cols)


def update_kernel(factor, divisor, merged_ref, square_ref, o_ref):
    scale = lax.rsqrt(square_ref[0:1, 0:1] * factor + EPS) * divisor
    o_ref[...] = (merged_ref[...] * scale).astype(o_ref.dtype)


def scaled(merged, squares, factor, divisor):
    return pl.pallas_call(
        functools.partial(update_kernel, factor, divisor),
        in_specs=[VMEM, VMEM],
        out_specs=VMEM,
        out_shape=jax.ShapeDtypeStruct(merged.shape, bf16),
        compiler_params=params(8),
        cost_estimate=cost(10**7, 4 * MIB),
        name="scaled",
    )(merged, squares)


def shards(replicas, shards_count, activations, cotangents, momentum, keep_index):
    activations, cotangents, momentum = activations[0], cotangents[0], momentum[0]
    rows, kv = momentum.shape
    rows_f, cols_f, rows_t = (jnp.asarray(t) for t in tables())

    mine = lax.axis_index("fsdp").astype(jnp.int32).reshape(1)
    replica = lax.axis_index("replica")
    near = [(i, i ^ 1) for i in range(shards_count)]
    cross = [(i, i ^ 2) for i in range(shards_count)]

    index = keep_index.transpose(0, 2, 1)
    own_index = lax.dynamic_index_in_dim(index, replica, 0, keepdims=False)

    part = first_product(mine, activations, cotangents, rows)
    cross_index = lax.ppermute(own_index, "fsdp", cross)
    got = lax.ppermute(part, "fsdp", near)
    part = held_product(2, mine, activations, cotangents, rows, f32)
    first, second = add_round(part, got, (GROUP, rows - GROUP))
    bulk_first = lax.ppermute(first, "fsdp", cross)
    cross_kept = kept_cross((first, second), cross_index, rows_f, cols_f)
    second, cross_kept = lax.optimization_barrier((second, cross_kept))
    cross_kept = lax.ppermute(cross_kept, "fsdp", cross)
    bulk_second = lax.ppermute(second, "fsdp", cross)

    part = held_product(1, mine, activations, cotangents, rows, bf16)
    got = lax.ppermute(part, "fsdp", near)
    part = held_product(0, mine, activations, cotangents, rows, f32)
    moment, kept = kept_own(part, got, momentum, own_index, cross_kept, rows_f, cols_f)

    pieces = [kept[None]]
    bit = 1
    while bit < replicas:
        held = pieces[0] if len(pieces) == 1 else jnp.concatenate(pieces)
        shifts = [bit] if bit == 1 or 2 * bit >= replicas else [bit, 2 * bit, 3 * bit]
        pieces = [held] + [lax.ppermute(held, "replica", [(i, i ^ shift) for i in range(replicas)]) for shift in shifts]
        bit *= len(shifts) + 1

    remaining = drop_sent(moment, kept, own_index, rows_t, cols_f)
    summed, squares = sum_replicas(replica.astype(jnp.int32).reshape(1), index, pieces, rows, kv)
    squares = squares + lax.ppermute(squares, "fsdp", near)
    squares = squares + lax.ppermute(squares, "fsdp", cross)
    merged = inverse(summed, rows_t, cols_f)
    count = float(shards_count * rows * kv) * float(replicas) ** 2
    update = scaled(merged, squares, 1.0 / count, 1.0 / replicas)
    new_momentum = remaining + jnp.concatenate([bulk_first, bulk_second]).astype(f32)
    return new_momentum[None], update


def solution(mesh):
    in_specs = (
        P("replica", "fsdp", None),
        P("replica", "fsdp", None),
        P("replica", "fsdp", None),
        P(None, "fsdp", None),
    )
    out_specs = (P("replica", "fsdp", None), P("fsdp", None))
    body = functools.partial(shards, mesh.shape["replica"], mesh.shape["fsdp"])
    return jax.shard_map(body, mesh=mesh, in_specs=in_specs, out_specs=out_specs, check_vma=False)
```
